128 devices in a mesh: dev: 128 (over z, y, x, core).
Axes of the slice: x: 4, y: 4, z: 4, core: 2. Of those that a mesh axis runs over, the one named last changes fastest.
Arguments:
- embeddings: float32 [32768, 1024], P('dev'), may hold values from -6 to 6
- lists: int32 [32768], P('dev'), may hold values from 0 to 65535, as said below
- row_ids: int32 [32768], P('dev'), may hold values from 0 to 32767, each once
- centroids: float32 [65536, 1024], P('dev'), may hold values from -6 to 6
- rotation: float32 [1024, 1024], replicated, may hold values from -0.1875 to 0.1875
Outputs:
- packed: float32 [65536, 1024], P('dev')
- packed_ids: int32 [65536], P('dev')
- list_offsets: int32 [65536], P('dev')
The draws below stay inside these ranges and needn't reach their ends.
Inputs may be any that keep to these rules, and one draw needn't show every extreme that they name: Lists l * 512 to (l + 1) * 512 - 1 belong to owner l. Among the rows of one device, at most 4 have lists of one owner, so an owner receives at most 512 rows; in every draw some owner receives exactly 4 rows from every device. `row_ids`: all identifiers are distinct.
All inputs are finite; a program needn't handle non-finite values.
Results may differ from the reference program's by a relative error of at most 0.0003.
Values sent between devices are 32-bit elements; how exact they have to be, the bound alone decides.
A program may use at most 64 MiB of HBM per device.

```python
import jax
import jax.numpy as jnp
from jax import lax

D = 1024
LISTS = 65536
ROWS_DEV = 256
TOTAL = 32768
LISTS_DEV = 512
SLOTS = 4
CAP = 512
N_DEV = 128


def draw_lists(key, part):
    full_key = jax.random.fold_in(key, 11)
    crowded = jax.random.randint(full_key, (), 0, N_DEV).astype(jnp.int32)

    def one_block(block_key):
        first_key = jax.random.fold_in(block_key, 1)
        second_key = jax.random.fold_in(block_key, 2)
        third_key = jax.random.fold_in(block_key, 3)
        shuffled = jax.random.permutation(first_key, (N_DEV - 1) * SLOTS).astype(jnp.int32)
        others = shuffled // SLOTS
        others = others + (others >= crowded).astype(jnp.int32)
        owners = jnp.concatenate([jnp.full((SLOTS,), 1, jnp.int32) * crowded, others[:ROWS_DEV - SLOTS]])
        mixing = jax.random.permutation(second_key, ROWS_DEV).astype(jnp.int32)
        owners = owners[mixing]
        inside = jax.random.randint(third_key, (ROWS_DEV,), 0, LISTS_DEV).astype(jnp.int32)
        return owners * LISTS_DEV + inside
    block_keys = jax.random.split(jax.random.fold_in(key, 12), N_DEV)
    return jax.vmap(one_block)(block_keys).reshape(-1).astype(jnp.int32)


def shard_levels(rng, dims, cuts, least, high):
    level = 1.0
    for axis_at, shards_of in cuts:
        steps = jax.random.uniform(jax.random.fold_in(jax.random.fold_in(rng, 6), axis_at), (shards_of,), jnp.float32, least / len(cuts), high / len(cuts))
        level = level * jnp.repeat(jnp.exp(steps), dims[axis_at] // shards_of).reshape((-1,) + (1,) * (len(dims) - 1 - axis_at))
    return level


def centred(own_key, shape, spread, most, cuts=(), held_as=jnp.bfloat16):
    gain = shard_levels(own_key, shape, cuts, -0.22, 0.18) if cuts else 1.0
    array = jax.random.normal(own_key, shape, jnp.float32) * spread * gain
    return jnp.minimum(jnp.maximum(array, -most), most).astype(held_as)


def setup_inputs(seed: int = 0) -> dict:
    key_of = jax.random.split(jax.random.key(seed), 6)
    return {
        "embeddings": centred(key_of[0], (TOTAL, D), 1.0, 6.0, ((0, 128),), jnp.float32),
        "lists": draw_lists(jax.random.fold_in(key_of[5], 71), 0),
        "row_ids": jax.random.permutation(key_of[2], TOTAL).astype(jnp.int32),
        "centroids": centred(key_of[3], (LISTS, D), 1.0, 6.0, ((0, 128),), jnp.float32),
        "rotation": centred(key_of[4], (D, D), D ** -0.5, 0.1875, (), jnp.float32),
    }


def reference(embeddings, lists, row_ids, centroids, rotation):
    total_rows = lists.shape[0]
    residual = embeddings - centroids[lists]
    transformed = jnp.dot(residual, rotation, precision=lax.Precision.HIGHEST, preferred_element_type=jnp.float32)
    sorted_order = jnp.argsort(lists, stable=True).astype(jnp.int32)
    sorted_lists = lists[sorted_order]
    owner_sorted = (sorted_lists // LISTS_DEV).astype(jnp.int32)
    owner_counts = jnp.zeros((N_DEV,), jnp.int32).at[owner_sorted].add(1)
    owner_first = (jnp.cumsum(owner_counts) - owner_counts).astype(jnp.int32)
    positions = jnp.arange(total_rows, dtype=jnp.int32) - owner_first[owner_sorted]
    destination = (owner_sorted * CAP + positions).astype(jnp.int32)
    packed = jnp.zeros((N_DEV * CAP, D), jnp.float32).at[destination].set(transformed[sorted_order])
    packed_ids = jnp.full((N_DEV * CAP,), -1, jnp.int32).at[destination].set(row_ids[sorted_order])
    totals = jnp.zeros((LISTS,), jnp.int32).at[lists].add(1)
    tiled_totals = totals.reshape(N_DEV, LISTS_DEV)
    list_offsets = (jnp.cumsum(tiled_totals, axis=1) - tiled_totals).reshape(-1).astype(jnp.int32)
    return packed, packed_ids, list_offsets
```

```python
import functools
import random

import jax
import jax.numpy as jnp
from jax import lax
from jax.experimental import pallas as pl
from jax.experimental.pallas import tpu as pltpu
from jax.sharding import PartitionSpec as P

MESH = pl.DeviceIdType.MESH
DIMS = (4, 4, 4, 2)
N = 128
SLOTS = 4
F32 = jnp.float32
BF16 = jnp.bfloat16
BIG = float(1 << 20)


def digits(k):
    return k // 32, k // 8 % 4, k // 2 % 4, k % 2


def hops(k):
    return sum((0, 1, 2, 1)[d] for d in digits(k)[:3])


def send_order():
    ks = list(range(1, N))
    random.Random(1).shuffle(ks)
    return sorted(ks, key=lambda k: -hops(k))


def iota(shape, dim):
    return lax.broadcasted_iota(jnp.int32, shape, dim)


def split3(x):
    hi = x.astype(BF16)
    rest = x - hi.astype(F32)
    mid = rest.astype(BF16)
    low = (rest - mid.astype(F32)).astype(BF16)
    return hi, mid, low


def split2(x):
    hi = x.astype(BF16)
    return hi, (x - hi.astype(F32)).astype(BF16)


def mm(a, b):
    return jnp.dot(a, b, preferred_element_type=F32)


def kernel(lists_ref, ids_ref, emb_hbm, cent_hbm, rot_hbm, packed_ref, pids_ref, offs_ref,
           emb, cent, rot, rot_hi, rot_lo, send, recv, msend, mrecv, cg, pos,
           lsem, ssem, rsem, msem):
    me = lax.axis_index("dev")
    emb_copy = pltpu.make_async_copy(emb_hbm, emb, lsem.at[0])
    cent_copy = pltpu.make_async_copy(cent_hbm, cent, lsem.at[1])
    rot_copy = pltpu.make_async_copy(rot_hbm, rot, lsem.at[2])
    emb_copy.start()
    cent_copy.start()
    rot_copy.start()

    barrier = pltpu.get_barrier_semaphore()
    for k in range(1, N):
        peer = me + k
        peer = jnp.where(peer >= N, peer - N, peer)
        pl.semaphore_signal(barrier, inc=1, device_id=(peer,), device_id_type=MESH)

    z, y, x, c = digits(me)
    zs = [((z + d) % 4) * 32 for d in range(4)]
    ys = [((y + d) % 4) * 8 for d in range(4)]
    xs = [((x + d) % 4) * 2 for d in range(4)]
    cs = [c, 1 - c]

    def peer_of(k):
        a, b, e, f = digits(k)
        return zs[a] + ys[b] + xs[e] + cs[f]

    order = send_order()

    rows = lists_ref.shape[1]
    owned = cent.shape[0]
    lists = lists_ref[...]
    owner = lists // owned
    local = (lists - owner * owned).astype(F32)
    ids = ids_ref[...].astype(F32)
    mine = owner == iota((N, rows), 0)
    earlier = (iota((rows, rows), 0) < iota((rows, rows), 1)).astype(BF16)
    count = mm(mine.astype(BF16), earlier)
    lane = iota((N, 128), 1)
    meta = jnp.zeros((N, 128), F32)
    picks = []
    for s in range(SLOTS):
        pick = mine & (count == float(s))
        l_of = jnp.sum(jnp.where(pick, local + 1.0, 0.0), axis=1, keepdims=True) - 1.0
        i_of = jnp.sum(jnp.where(pick, ids, 0.0), axis=1, keepdims=True)
        meta = jnp.where(lane == s, l_of, meta)
        meta = jnp.where(lane == SLOTS + s, i_of, meta)
        picks.append(pick.astype(BF16))
    msend[...] = meta.reshape(N, 1, 128)
    pick_all = jnp.concatenate(picks, axis=0)

    emb_copy.wait()
    width = emb.shape[1]
    for nb in range(width // 256):
        hi, mid, low = split3(emb[:, nb * 256:(nb + 1) * 256])
        out = mm(pick_all, hi) + mm(pick_all, mid) + mm(pick_all, low)
        for j in range(2):
            send[pl.ds(nb * 2 + j, SLOTS * N, stride=8), :] = out[:, j * 128:(j + 1) * 128]

    mrecv[pl.ds(me, 1)] = msend[pl.ds(me, 1)]
    for s in range(SLOTS):
        at = pl.ds(pl.multiple_of((s * N + me) * 8, 8), 8)
        recv[at, :] = send[at, :]

    pl.semaphore_wait(barrier, N - 1)
    for k in order:
        peer = peer_of(k)
        pltpu.make_async_remote_copy(
            src_ref=msend.at[pl.ds(peer, 1)], dst_ref=mrecv.at[pl.ds(me, 1)],
            send_sem=msem.at[0], recv_sem=msem.at[1], device_id=(peer,), device_id_type=MESH,
        ).start()

    def send_slot(s, carry):
        for k in order:
            peer = peer_of(k)
            pltpu.make_async_remote_copy(
                src_ref=send.at[pl.ds(pl.multiple_of((s * N + peer) * 8, 8), 8)],
                dst_ref=recv.at[pl.ds(pl.multiple_of((s * N + me) * 8, 8), 8)],
                send_sem=ssem.at[0], recv_sem=rsem.at[s], device_id=(peer,), device_id_type=MESH,
            ).start()
        return carry

    lax.fori_loop(0, SLOTS, send_slot, 0)

    rot_copy.wait()
    for nb in range(width // 256):
        at = slice(nb * 256, (nb + 1) * 256)
        hi, low = split2(rot[:, at])
        rot_hi[:, at] = hi
        rot_lo[:, at] = low

    m_all = msend.at[pl.ds(0, N - 1)]
    pltpu.make_async_copy(m_all, m_all, msem.at[1]).wait()
    got = mrecv[...].reshape(N, 128)
    got_t = got.T
    src_col = iota((N, 1), 0).astype(F32)
    src_row = iota((1, N), 1).astype(F32)
    list_cols = [got[:, s:s + 1] for s in range(SLOTS)]
    list_rows = [got_t[s:s + 1, :] for s in range(SLOTS)]

    def keys(lists_of, src):
        return [jnp.where(v >= 0, v * float(SLOTS * N) + src * float(SLOTS) + float(s), BIG)
                for s, v in enumerate(lists_of)]

    key_cols = keys(list_cols, src_col)
    key_rows = keys(list_rows, src_row)
    q_lane = iota((N, owned), 1).astype(F32)
    pid = jnp.zeros((1, owned), F32)
    off = jnp.zeros((1, owned), F32)
    for s in range(SLOTS):
        by_row = jnp.zeros((N, N), F32)
        by_col = jnp.zeros((N, N), F32)
        for t in range(SLOTS):
            by_row += (key_cols[t] < key_rows[s]).astype(F32)
            by_col += (key_rows[t] < key_cols[s]).astype(F32)
        at_row = jnp.where(list_rows[s] >= 0, jnp.sum(by_row, axis=0, keepdims=True), BIG)
        at_col = jnp.where(list_cols[s] >= 0, jnp.sum(by_col, axis=1, keepdims=True), BIG)
        pos[s:s + 1, :] = at_row
        id_col = got[:, SLOTS + s:SLOTS + s + 1] + 1.0
        pid += jnp.sum(jnp.where(at_col == q_lane, id_col, 0.0), axis=0, keepdims=True)
        off += jnp.sum((key_cols[s] < q_lane * float(SLOTS * N)).astype(F32), axis=0, keepdims=True)
    pids_ref[...] = (pid - 1.0).astype(jnp.int32)
    offs_ref[...] = off.astype(jnp.int32)

    cent_copy.wait()
    onehot = jnp.concatenate([(v == q_lane).astype(BF16) for v in list_cols], axis=0)
    for nb in range(width // 256):
        hi, mid, low = split3(cent[:, nb * 256:(nb + 1) * 256])
        cg[:, nb * 256:(nb + 1) * 256] = mm(onehot, hi) + mm(onehot, mid) + mm(onehot, low)

    packed_ref[...] = jnp.zeros(packed_ref.shape, F32)
    q_sub = iota((SLOTS * N, N), 0).astype(F32)

    def chunk(s, carry):
        r_all = recv.at[pl.ds(0, (N - 1) * 8)]
        pltpu.make_async_copy(r_all, r_all, rsem.at[s]).wait()
        parts = [recv[pl.ds(s * (N * 8) + j, N, stride=8), :] for j in range(8)]
        resid = jnp.concatenate(parts, axis=1) - cg[pl.ds(pl.multiple_of(s * N, N), N), :]
        hi, low = split2(resid)
        both = jnp.concatenate([hi, low], axis=0)
        place = (pos[pl.ds(s, 1), :] == q_sub).astype(BF16)
        place2 = jnp.concatenate([place, place], axis=1)
        for nb in range(width // 256):
            at = slice(nb * 256, (nb + 1) * 256)
            first = mm(both, rot_hi[:, at])
            turned = first[:N] + first[N:] + mm(hi, rot_lo[:, at])
            t_hi, t_lo = split2(turned)
            packed_ref[:, at] += mm(place2, jnp.concatenate([t_hi, t_lo], axis=0))
        return carry

    lax.fori_loop(0, SLOTS, chunk, 0)
    s_all = send.at[pl.ds(0, SLOTS * (N - 1) * 8)]
    pltpu.make_async_copy(s_all, s_all, ssem.at[0]).wait()
    pltpu.make_async_copy(m_all, m_all, msem.at[0]).wait()


def local(embeddings, lists, row_ids, centroids, rotation):
    rows, width = embeddings.shape
    owned = centroids.shape[0]
    slots = SLOTS * N
    vm = pl.BlockSpec(memory_space=pltpu.VMEM)
    hbm = pl.BlockSpec(memory_space=pl.ANY)
    packed, pids, offs = pl.pallas_call(
        kernel,
        name="exchange",
        out_shape=(
            jax.ShapeDtypeStruct((slots, width), F32),
            jax.ShapeDtypeStruct((1, slots), jnp.int32),
            jax.ShapeDtypeStruct((1, owned), jnp.int32),
        ),
        in_specs=[vm, vm, hbm, hbm, hbm],
        out_specs=(vm, vm, vm),
        scratch_shapes=[
            pltpu.VMEM((rows, width), F32),
            pltpu.VMEM((owned, width), F32),
            pltpu.VMEM((width, width), F32),
            pltpu.VMEM((width, width), BF16),
            pltpu.VMEM((width, width), BF16),
            pltpu.VMEM((slots * 8, 128), F32),
            pltpu.VMEM((slots * 8, 128), F32),
            pltpu.VMEM((N, 1, 128), F32),
            pltpu.VMEM((N, 1, 128), F32),
            pltpu.VMEM((slots, width), F32),
            pltpu.VMEM((8, 128), F32),
            pltpu.SemaphoreType.DMA((3,)),
            pltpu.SemaphoreType.DMA((1,)),
            pltpu.SemaphoreType.DMA((SLOTS,)),
            pltpu.SemaphoreType.DMA((2,)),
        ],
        compiler_params=pltpu.CompilerParams(
            collective_id=0, has_side_effects=True, vmem_limit_bytes=40 << 20
        ),
    )(lists.reshape(1, rows), row_ids.reshape(1, rows), embeddings, centroids, rotation)
    return packed, pids.reshape(-1), offs.reshape(-1)


def solution(mesh):
    in_specs = (P("dev", None), P("dev"), P("dev"), P("dev", None), P())
    out_specs = (P("dev", None), P("dev"), P("dev"))
    return jax.shard_map(local, mesh=mesh, in_specs=in_specs, out_specs=out_specs, check_vma=False)
```

```python
import functools
import random

import jax
import jax.numpy as jnp
from jax import lax
from jax.experimental import pallas as pl
from jax.experimental.pallas import tpu as pltpu
from jax.sharding import PartitionSpec as P

MESH = pl.DeviceIdType.MESH
DIMS = (4, 4, 4, 2)
N = 128
SLOTS = 4
F32 = jnp.float32
BF16 = jnp.bfloat16
BIG = float(1 << 20)


def digits(k):
    return k // 32, k // 8 % 4, k // 2 % 4, k % 2


def hops(k):
    return sum((0, 1, 2, 1)[d] for d in digits(k)[:3])


def send_order():
    ks = list(range(1, N))
    random.Random(1).shuffle(ks)
    return sorted(ks, key=lambda k: -hops(k))


def iota(shape, dim):
    return lax.broadcasted_iota(jnp.int32, shape, dim)


def split3(x):
    hi = x.astype(BF16)
    rest = x - hi.astype(F32)
    mid = rest.astype(BF16)
    low = (rest - mid.astype(F32)).astype(BF16)
    return hi, mid, low


def split2(x):
    hi = x.astype(BF16)
    return hi, (x - hi.astype(F32)).astype(BF16)


def mm(a, b):
    return jnp.dot(a, b, preferred_element_type=F32)


def kernel(lists_hbm, ids_hbm, emb_hbm, cent_hbm, rot_hbm, packed_ref, pids_ref, offs_ref,
           lists_ref, ids_ref, emb, cent, rot, rot_hi, rot_lo, send, recv, msend, mrecv, cg, pos,
           lsem, ssem, rsem, msem):
    me = lax.axis_index("dev")
    lists_copy = pltpu.make_async_copy(lists_hbm, lists_ref, lsem.at[3])
    ids_copy = pltpu.make_async_copy(ids_hbm, ids_ref, lsem.at[4])
    emb_copy = pltpu.make_async_copy(emb_hbm, emb, lsem.at[0])
    cent_copy = pltpu.make_async_copy(cent_hbm, cent, lsem.at[1])
    rot_copy = pltpu.make_async_copy(rot_hbm, rot, lsem.at[2])
    lists_copy.start()
    ids_copy.start()
    emb_copy.start()

    barrier = pltpu.get_barrier_semaphore()
    for k in range(1, N):
        peer = me + k
        peer = jnp.where(peer >= N, peer - N, peer)
        pl.semaphore_signal(barrier, inc=1, device_id=(peer,), device_id_type=MESH)

    z, y, x, c = digits(me)
    zs = [((z + d) % 4) * 32 for d in range(4)]
    ys = [((y + d) % 4) * 8 for d in range(4)]
    xs = [((x + d) % 4) * 2 for d in range(4)]
    cs = [c, 1 - c]

    def peer_of(k):
        a, b, e, f = digits(k)
        return zs[a] + ys[b] + xs[e] + cs[f]

    order = send_order()

    rows = lists_ref.shape[1]
    owned = cent.shape[0]
    lists_copy.wait()
    ids_copy.wait()
    lists = lists_ref[...]
    owner = lists // owned
    local = (lists - owner * owned).astype(F32)
    ids = ids_ref[...].astype(F32)
    mine = owner == iota((N, rows), 0)
    earlier = (iota((rows, rows), 0) < iota((rows, rows), 1)).astype(BF16)
    count = mm(mine.astype(BF16), earlier)
    lane = iota((N, 128), 1)
    meta = jnp.zeros((N, 128), F32)
    picks = []
    for s in range(SLOTS):
        pick = mine & (count == float(s))
        l_of = jnp.sum(jnp.where(pick, local + 1.0, 0.0), axis=1, keepdims=True) - 1.0
        i_of = jnp.sum(jnp.where(pick, ids, 0.0), axis=1, keepdims=True)
        meta = jnp.where(lane == s, l_of, meta)
        meta = jnp.where(lane == SLOTS + s, i_of, meta)
        picks.append(pick.astype(BF16))
    msend[...] = meta.reshape(N, 1, 128)
    pick_all = jnp.concatenate(picks, axis=0)

    emb_copy.wait()
    rot_copy.start()
    cent_copy.start()
    width = emb.shape[1]
    for nb in range(width // 256):
        hi, mid, low = split3(emb[:, nb * 256:(nb + 1) * 256])
        out = mm(pick_all, hi) + mm(pick_all, mid) + mm(pick_all, low)
        for j in range(2):
            send[pl.ds(nb * 2 + j, SLOTS * N, stride=8), :] = out[:, j * 128:(j + 1) * 128]

    mrecv[pl.ds(me, 1)] = msend[pl.ds(me, 1)]
    for s in range(SLOTS):
        at = pl.ds(pl.multiple_of((s * N + me) * 8, 8), 8)
        recv[at, :] = send[at, :]

    pl.semaphore_wait(barrier, N - 1)
    for k in order:
        peer = peer_of(k)
        pltpu.make_async_remote_copy(
            src_ref=msend.at[pl.ds(peer, 1)], dst_ref=mrecv.at[pl.ds(me, 1)],
            send_sem=msem.at[0], recv_sem=msem.at[1], device_id=(peer,), device_id_type=MESH,
        ).start()

    def send_slot(s, carry):
        for k in order:
            peer = peer_of(k)
            pltpu.make_async_remote_copy(
                src_ref=send.at[pl.ds(pl.multiple_of((s * N + peer) * 8, 8), 8)],
                dst_ref=recv.at[pl.ds(pl.multiple_of((s * N + me) * 8, 8), 8)],
                send_sem=ssem.at[0], recv_sem=rsem.at[s], device_id=(peer,), device_id_type=MESH,
            ).start()
        return carry

    lax.fori_loop(0, SLOTS, send_slot, 0)

    rot_copy.wait()
    for nb in range(width // 256):
        at = slice(nb * 256, (nb + 1) * 256)
        hi, low = split2(rot[:, at])
        rot_hi[:, at] = hi
        rot_lo[:, at] = low

    m_all = msend.at[pl.ds(0, N - 1)]
    pltpu.make_async_copy(m_all, m_all, msem.at[1]).wait()
    got = mrecv[...].reshape(N, 128)
    got_t = got.T
    src_col = iota((N, 1), 0).astype(F32)
    src_row = iota((1, N), 1).astype(F32)
    list_cols = [got[:, s:s + 1] for s in range(SLOTS)]
    list_rows = [got_t[s:s + 1, :] for s in range(SLOTS)]

    def keys(lists_of, src):
        return [jnp.where(v >= 0, v * float(SLOTS * N) + src * float(SLOTS) + float(s), BIG)
                for s, v in enumerate(lists_of)]

    key_cols = keys(list_cols, src_col)
    key_rows = keys(list_rows, src_row)
    q_lane = iota((N, owned), 1).astype(F32)
    pid = jnp.zeros((1, owned), F32)
    off = jnp.zeros((1, owned), F32)
    for s in range(SLOTS):
        by_row = jnp.zeros((N, N), F32)
        by_col = jnp.zeros((N, N), F32)
        for t in range(SLOTS):
            by_row += (key_cols[t] < key_rows[s]).astype(F32)
            by_col += (key_rows[t] < key_cols[s]).astype(F32)
        at_row = jnp.where(list_rows[s] >= 0, jnp.sum(by_row, axis=0, keepdims=True), BIG)
        at_col = jnp.where(list_cols[s] >= 0, jnp.sum(by_col, axis=1, keepdims=True), BIG)
        pos[s:s + 1, :] = at_row
        id_col = got[:, SLOTS + s:SLOTS + s + 1] + 1.0
        pid += jnp.sum(jnp.where(at_col == q_lane, id_col, 0.0), axis=0, keepdims=True)
        off += jnp.sum((key_cols[s] < q_lane * float(SLOTS * N)).astype(F32), axis=0, keepdims=True)
    pids_ref[...] = (pid - 1.0).astype(jnp.int32)
    offs_ref[...] = off.astype(jnp.int32)

    cent_copy.wait()
    onehot = jnp.concatenate([(v == q_lane).astype(BF16) for v in list_cols], axis=0)
    for nb in range(width // 256):
        hi, mid, low = split3(cent[:, nb * 256:(nb + 1) * 256])
        cg[:, nb * 256:(nb + 1) * 256] = mm(onehot, hi) + mm(onehot, mid) + mm(onehot, low)

    packed_ref[...] = jnp.zeros(packed_ref.shape, F32)
    q_sub = iota((SLOTS * N, N), 0).astype(F32)

    def chunk(s, carry):
        r_all = recv.at[pl.ds(0, (N - 1) * 8)]
        pltpu.make_async_copy(r_all, r_all, rsem.at[s]).wait()
        parts = [recv[pl.ds(s * (N * 8) + j, N, stride=8), :] for j in range(8)]
        resid = jnp.concatenate(parts, axis=1) - cg[pl.ds(pl.multiple_of(s * N, N), N), :]
        hi, low = split2(resid)
        both = jnp.concatenate([hi, low], axis=0)
        place = (pos[pl.ds(s, 1), :] == q_sub).astype(BF16)
        place2 = jnp.concatenate([place, place], axis=1)
        for nb in range(width // 256):
            at = slice(nb * 256, (nb + 1) * 256)
            first = mm(both, rot_hi[:, at])
            turned = first[:N] + first[N:] + mm(hi, rot_lo[:, at])
            t_hi, t_lo = split2(turned)
            packed_ref[:, at] += mm(place2, jnp.concatenate([t_hi, t_lo], axis=0))
        return carry

    lax.fori_loop(0, SLOTS, chunk, 0)
    s_all = send.at[pl.ds(0, SLOTS * (N - 1) * 8)]
    pltpu.make_async_copy(s_all, s_all, ssem.at[0]).wait()
    pltpu.make_async_copy(m_all, m_all, msem.at[0]).wait()


def write_out(packed_vm, pids_vm, offs_vm, packed_ref, pids_ref, offs_ref, sem):
    pairs = ((packed_vm, packed_ref), (pids_vm, pids_ref), (offs_vm, offs_ref))
    copies = [pltpu.make_async_copy(a, b, sem.at[i]) for i, (a, b) in enumerate(pairs)]
    for copy in copies:
        copy.start()
    for copy in copies:
        copy.wait()


def local(embeddings, lists, row_ids, centroids, rotation):
    rows, width = embeddings.shape
    owned = centroids.shape[0]
    slots = SLOTS * N
    vm = pl.BlockSpec(memory_space=pltpu.VMEM)
    hbm = pl.BlockSpec(memory_space=pltpu.HBM)
    results = (
        jax.ShapeDtypeStruct((slots, width), F32),
        jax.ShapeDtypeStruct((1, slots), jnp.int32),
        jax.ShapeDtypeStruct((1, owned), jnp.int32),
    )
    in_hbm = [
        pltpu.with_memory_space_constraint(v, pltpu.HBM)
        for v in (lists.reshape(1, rows), row_ids.reshape(1, rows), embeddings, centroids, rotation)
    ]
    held = pl.pallas_call(
        kernel,
        name="exchange",
        out_shape=results,
        in_specs=[hbm] * 5,
        out_specs=(vm, vm, vm),
        scratch_shapes=[
            pltpu.VMEM((1, rows), jnp.int32),
            pltpu.VMEM((1, rows), jnp.int32),
            pltpu.VMEM((rows, width), F32),
            pltpu.VMEM((owned, width), F32),
            pltpu.VMEM((width, width), F32),
            pltpu.VMEM((width, width), BF16),
            pltpu.VMEM((width, width), BF16),
            pltpu.VMEM((slots * 8, 128), F32),
            pltpu.VMEM((slots * 8, 128), F32),
            pltpu.VMEM((N, 1, 128), F32),
            pltpu.VMEM((N, 1, 128), F32),
            pltpu.VMEM((slots, width), F32),
            pltpu.VMEM((8, 128), F32),
            pltpu.SemaphoreType.DMA((5,)),
            pltpu.SemaphoreType.DMA((1,)),
            pltpu.SemaphoreType.DMA((SLOTS,)),
            pltpu.SemaphoreType.DMA((2,)),
        ],
        compiler_params=pltpu.CompilerParams(
            collective_id=0, has_side_effects=True, vmem_limit_bytes=40 << 20
        ),
    )(*in_hbm)
    packed, pids, offs = pl.pallas_call(
        write_out,
        name="write_out",
        out_shape=results,
        in_specs=[vm] * 3,
        out_specs=(hbm,) * 3,
        scratch_shapes=[pltpu.SemaphoreType.DMA((3,))],
        compiler_params=pltpu.CompilerParams(vmem_limit_bytes=4 << 20),
    )(*held)
    return packed, pids.reshape(-1), offs.reshape(-1)


def solution(mesh):
    in_specs = (P("dev", None), P("dev"), P("dev"), P("dev", None), P())
    out_specs = (P("dev", None), P("dev"), P("dev"))
    return jax.shard_map(local, mesh=mesh, in_specs=in_specs, out_specs=out_specs, check_vma=False)
```

```python
import functools
import random

import jax
import jax.numpy as jnp
from jax import lax
from jax.experimental import pallas as pl
from jax.experimental.pallas import tpu as pltpu
from jax.sharding import PartitionSpec as P

MESH = pl.DeviceIdType.MESH
DIMS = (4, 4, 4, 2)
N = 128
SLOTS = 4
F32 = jnp.float32
BF16 = jnp.bfloat16
BIG = float(1 << 20)


def digits(k):
    return k // 32, k // 8 % 4, k // 2 % 4, k % 2


def hops(k):
    return sum((0, 1, 2, 1)[d] for d in digits(k)[:3])


def send_order():
    ks = list(range(1, N))
    random.Random(1).shuffle(ks)
    return sorted(ks, key=lambda k: -hops(k))


def iota(shape, dim):
    return lax.broadcasted_iota(jnp.int32, shape, dim)


def split3(x):
    hi = x.astype(BF16)
    rest = x - hi.astype(F32)
    mid = rest.astype(BF16)
    low = (rest - mid.astype(F32)).astype(BF16)
    return hi, mid, low


def split2(x):
    hi = x.astype(BF16)
    return hi, (x - hi.astype(F32)).astype(BF16)


def mm(a, b):
    return jnp.dot(a, b, preferred_element_type=F32)


def kernel(lists_hbm, ids_hbm, emb_hbm, cent_hbm, rot_hbm, packed_ref, pids_ref, offs_ref,
           lists_ref, ids_ref, emb, cent, rot, rot_hi, rot_lo, send, recv, msend, mrecv, cg, pos, turned2,
           lsem, ssem, rsem, msem):
    me = lax.axis_index("dev")
    lists_copy = pltpu.make_async_copy(lists_hbm, lists_ref, lsem.at[3])
    ids_copy = pltpu.make_async_copy(ids_hbm, ids_ref, lsem.at[4])
    emb_copy = pltpu.make_async_copy(emb_hbm, emb, lsem.at[0])
    cent_copy = pltpu.make_async_copy(cent_hbm, cent, lsem.at[1])
    rot_copy = pltpu.make_async_copy(rot_hbm, rot, lsem.at[2])
    lists_copy.start()
    ids_copy.start()
    emb_copy.start()

    barrier = pltpu.get_barrier_semaphore()
    for k in range(1, N):
        peer = me + k
        peer = jnp.where(peer >= N, peer - N, peer)
        pl.semaphore_signal(barrier, inc=1, device_id=(peer,), device_id_type=MESH)

    z, y, x, c = digits(me)
    zs = [((z + d) % 4) * 32 for d in range(4)]
    ys = [((y + d) % 4) * 8 for d in range(4)]
    xs = [((x + d) % 4) * 2 for d in range(4)]
    cs = [c, 1 - c]

    def peer_of(k):
        a, b, e, f = digits(k)
        return zs[a] + ys[b] + xs[e] + cs[f]

    order = send_order()

    rows = lists_ref.shape[1]
    owned = cent.shape[0]
    lists_copy.wait()
    ids_copy.wait()
    lists = lists_ref[...]
    owner = lists // owned
    local = (lists - owner * owned).astype(F32)
    ids = ids_ref[...].astype(F32)
    mine = owner == iota((N, rows), 0)
    earlier = (iota((rows, rows), 0) < iota((rows, rows), 1)).astype(BF16)
    count = mm(mine.astype(BF16), earlier)
    lane = iota((N, 128), 1)
    meta = jnp.zeros((N, 128), F32)
    picks = []
    for s in range(SLOTS):
        pick = mine & (count == float(s))
        l_of = jnp.sum(jnp.where(pick, local + 1.0, 0.0), axis=1, keepdims=True) - 1.0
        i_of = jnp.sum(jnp.where(pick, ids, 0.0), axis=1, keepdims=True)
        meta = jnp.where(lane == s, l_of, meta)
        meta = jnp.where(lane == SLOTS + s, i_of, meta)
        picks.append(pick.astype(BF16))
    msend[...] = meta.reshape(N, 1, 128)
    pick_all = jnp.concatenate(picks, axis=0)

    emb_copy.wait()
    rot_copy.start()
    cent_copy.start()
    width = emb.shape[1]
    for nb in range(width // 256):
        hi, mid, low = split3(emb[:, nb * 256:(nb + 1) * 256])
        out = mm(pick_all, hi) + mm(pick_all, mid) + mm(pick_all, low)
        for j in range(2):
            send[pl.ds(nb * 2 + j, SLOTS * N, stride=8), :] = out[:, j * 128:(j + 1) * 128]

    mrecv[pl.ds(me, 1)] = msend[pl.ds(me, 1)]
    for s in range(SLOTS):
        at = pl.ds(pl.multiple_of((s * N + me) * 8, 8), 8)
        recv[at, :] = send[at, :]

    pl.semaphore_wait(barrier, N - 1)
    for k in order:
        peer = peer_of(k)
        pltpu.make_async_remote_copy(
            src_ref=msend.at[pl.ds(peer, 1)], dst_ref=mrecv.at[pl.ds(me, 1)],
            send_sem=msem.at[0], recv_sem=msem.at[1], device_id=(peer,), device_id_type=MESH,
        ).start()

    def send_slot(s, carry):
        for k in order:
            peer = peer_of(k)
            pltpu.make_async_remote_copy(
                src_ref=send.at[pl.ds(pl.multiple_of((s * N + peer) * 8, 8), 8)],
                dst_ref=recv.at[pl.ds(pl.multiple_of((s * N + me) * 8, 8), 8)],
                send_sem=ssem.at[0], recv_sem=rsem.at[s], device_id=(peer,), device_id_type=MESH,
            ).start()
        return carry

    lax.fori_loop(0, SLOTS, send_slot, 0)

    rot_copy.wait()
    for nb in range(width // 256):
        at = slice(nb * 256, (nb + 1) * 256)
        hi, low = split2(rot[:, at])
        rot_hi[:, at] = hi
        rot_lo[:, at] = low

    m_all = msend.at[pl.ds(0, N - 1)]
    pltpu.make_async_copy(m_all, m_all, msem.at[1]).wait()
    got = mrecv[...].reshape(N, 128)
    got_t = got.T
    src_col = iota((N, 1), 0).astype(F32)
    src_row = iota((1, N), 1).astype(F32)
    list_cols = [got[:, s:s + 1] for s in range(SLOTS)]
    list_rows = [got_t[s:s + 1, :] for s in range(SLOTS)]

    def keys(lists_of, src):
        return [jnp.where(v >= 0, v * float(SLOTS * N) + src * float(SLOTS) + float(s), BIG)
                for s, v in enumerate(lists_of)]

    key_cols = keys(list_cols, src_col)
    key_rows = keys(list_rows, src_row)
    q_lane = iota((N, owned), 1).astype(F32)
    pid = jnp.zeros((1, owned), F32)
    off = jnp.zeros((1, owned), F32)
    for s in range(SLOTS):
        by_row = jnp.zeros((N, N), F32)
        by_col = jnp.zeros((N, N), F32)
        for t in range(SLOTS):
            by_row += (key_cols[t] < key_rows[s]).astype(F32)
            by_col += (key_rows[t] < key_cols[s]).astype(F32)
        at_row = jnp.where(list_rows[s] >= 0, jnp.sum(by_row, axis=0, keepdims=True), BIG)
        at_col = jnp.where(list_cols[s] >= 0, jnp.sum(by_col, axis=1, keepdims=True), BIG)
        pos[s:s + 1, :] = at_row
        id_col = got[:, SLOTS + s:SLOTS + s + 1] + 1.0
        pid += jnp.sum(jnp.where(at_col == q_lane, id_col, 0.0), axis=0, keepdims=True)
        off += jnp.sum((key_cols[s] < q_lane * float(SLOTS * N)).astype(F32), axis=0, keepdims=True)
    pids_ref[...] = (pid - 1.0).astype(jnp.int32)
    offs_ref[...] = off.astype(jnp.int32)

    cent_copy.wait()
    onehot = jnp.concatenate([(v == q_lane).astype(BF16) for v in list_cols], axis=0)
    for nb in range(width // 256):
        hi, mid, low = split3(cent[:, nb * 256:(nb + 1) * 256])
        cg[:, nb * 256:(nb + 1) * 256] = mm(onehot, hi) + mm(onehot, mid) + mm(onehot, low)

    packed_ref[...] = jnp.zeros(packed_ref.shape, F32)
    q_sub = iota((SLOTS * N, N), 0).astype(F32)

    def chunk(s, carry):
        r_all = recv.at[pl.ds(0, (N - 1) * 8)]
        pltpu.make_async_copy(r_all, r_all, rsem.at[s]).wait()
        parts = [recv[pl.ds(s * (N * 8) + j, N, stride=8), :] for j in range(8)]
        resid = jnp.concatenate(parts, axis=1) - cg[pl.ds(pl.multiple_of(s * N, N), N), :]
        hi, low = split2(resid)
        both = jnp.concatenate([hi, low], axis=0)
        place = (pos[pl.ds(s, 1), :] == q_sub).astype(BF16)
        place2 = jnp.concatenate([place, place], axis=1)
        for nb in range(width // 256):
            at = slice(nb * 256, (nb + 1) * 256)
            first = mm(both, rot_hi[:, at])
            turned = first[:N] + first[N:] + mm(hi, rot_lo[:, at])
            t_hi, t_lo = split2(turned)
            turned2[0:N, at] = t_hi
            turned2[N:, at] = t_lo
        packed_ref[...] += mm(place2, turned2[...])
        return carry

    lax.fori_loop(0, SLOTS, chunk, 0)
    s_all = send.at[pl.ds(0, SLOTS * (N - 1) * 8)]
    pltpu.make_async_copy(s_all, s_all, ssem.at[0]).wait()
    pltpu.make_async_copy(m_all, m_all, msem.at[0]).wait()


def write_out(packed_vm, pids_vm, offs_vm, packed_ref, pids_ref, offs_ref, sem):
    pairs = ((packed_vm, packed_ref), (pids_vm, pids_ref), (offs_vm, offs_ref))
    copies = [pltpu.make_async_copy(a, b, sem.at[i]) for i, (a, b) in enumerate(pairs)]
    for copy in copies:
        copy.start()
    for copy in copies:
        copy.wait()


def local(embeddings, lists, row_ids, centroids, rotation):
    rows, width = embeddings.shape
    owned = centroids.shape[0]
    slots = SLOTS * N
    vm = pl.BlockSpec(memory_space=pltpu.VMEM)
    hbm = pl.BlockSpec(memory_space=pltpu.HBM)
    results = (
        jax.ShapeDtypeStruct((slots, width), F32),
        jax.ShapeDtypeStruct((1, slots), jnp.int32),
        jax.ShapeDtypeStruct((1, owned), jnp.int32),
    )
    in_hbm = [
        pltpu.with_memory_space_constraint(v, pltpu.HBM)
        for v in (lists.reshape(1, rows), row_ids.reshape(1, rows), embeddings, centroids, rotation)
    ]
    held = pl.pallas_call(
        kernel,
        name="exchange",
        out_shape=results,
        in_specs=[hbm] * 5,
        out_specs=(vm, vm, vm),
        scratch_shapes=[
            pltpu.VMEM((1, rows), jnp.int32),
            pltpu.VMEM((1, rows), jnp.int32),
            pltpu.VMEM((rows, width), F32),
            pltpu.VMEM((owned, width), F32),
            pltpu.VMEM((width, width), F32),
            pltpu.VMEM((width, width), BF16),
            pltpu.VMEM((width, width), BF16),
            pltpu.VMEM((slots * 8, 128), F32),
            pltpu.VMEM((slots * 8, 128), F32),
            pltpu.VMEM((N, 1, 128), F32),
            pltpu.VMEM((N, 1, 128), F32),
            pltpu.VMEM((slots, width), F32),
            pltpu.VMEM((8, 128), F32),
            pltpu.VMEM((2 * N, width), BF16),
            pltpu.SemaphoreType.DMA((5,)),
            pltpu.SemaphoreType.DMA((1,)),
            pltpu.SemaphoreType.DMA((SLOTS,)),
            pltpu.SemaphoreType.DMA((2,)),
        ],
        compiler_params=pltpu.CompilerParams(
            collective_id=0, has_side_effects=True, vmem_limit_bytes=40 << 20
        ),
    )(*in_hbm)
    packed, pids, offs = pl.pallas_call(
        write_out,
        name="write_out",
        out_shape=results,
        in_specs=[vm] * 3,
        out_specs=(hbm,) * 3,
        scratch_shapes=[pltpu.SemaphoreType.DMA((3,))],
        compiler_params=pltpu.CompilerParams(vmem_limit_bytes=4 << 20),
    )(*held)
    return packed, pids.reshape(-1), offs.reshape(-1)


def solution(mesh):
    in_specs = (P("dev", None), P("dev"), P("dev"), P("dev", None), P())
    out_specs = (P("dev", None), P("dev"), P("dev"))
    return jax.shard_map(local, mesh=mesh, in_specs=in_specs, out_specs=out_specs, check_vma=False)
```

```python
import functools
import random

import jax
import jax.numpy as jnp
from jax import lax
from jax.experimental import pallas as pl
from jax.experimental.pallas import tpu as pltpu
from jax.sharding import PartitionSpec as P

MESH = pl.DeviceIdType.MESH
DIMS = (4, 4, 4, 2)
N = 128
SLOTS = 4
F32 = jnp.float32
BF16 = jnp.bfloat16
BIG = float(1 << 20)
NEAR_SLOTS = 3


def digits(k):
    return k // 32, k // 8 % 4, k // 2 % 4, k % 2


def hops(k):
    return sum((0, 1, 2, 1)[d] for d in digits(k)[:3])


def send_order():
    ks = list(range(1, N))
    random.Random(1).shuffle(ks)
    return sorted(ks, key=lambda k: -hops(k))


def iota(shape, dim):
    return lax.broadcasted_iota(jnp.int32, shape, dim)


def split3(x):
    hi = x.astype(BF16)
    rest = x - hi.astype(F32)
    mid = rest.astype(BF16)
    low = (rest - mid.astype(F32)).astype(BF16)
    return hi, mid, low


def split2(x):
    hi = x.astype(BF16)
    return hi, (x - hi.astype(F32)).astype(BF16)


def mm(a, b):
    return jnp.dot(a, b, preferred_element_type=F32)


def kernel(lists_hbm, ids_hbm, emb_hbm, cent_hbm, rot_hbm, packed_ref, pids_ref, offs_ref,
           lists_ref, ids_ref, emb, cent, rot, rot_hi, rot_lo, send, recv, msend, mrecv, cg, pos, turned2,
           lsem, ssem, rsem, msem, wider):
    me = lax.axis_index("dev")
    lists_copy = pltpu.make_async_copy(lists_hbm, lists_ref, lsem.at[3])
    ids_copy = pltpu.make_async_copy(ids_hbm, ids_ref, lsem.at[4])
    emb_copy = pltpu.make_async_copy(emb_hbm, emb, lsem.at[0])
    cent_copy = pltpu.make_async_copy(cent_hbm, cent, lsem.at[1])
    rot_copy = pltpu.make_async_copy(rot_hbm, rot, lsem.at[2])
    lists_copy.start()
    ids_copy.start()
    emb_copy.start()

    z, y, x, c = digits(me)
    zs = [((z + d) % 4) * 32 for d in range(4)]
    ys = [((y + d) % 4) * 8 for d in range(4)]
    xs = [((x + d) % 4) * 2 for d in range(4)]
    cs = [c, 1 - c]

    def peer_of(k):
        a, b, e, f = digits(k)
        return zs[a] + ys[b] + xs[e] + cs[f]

    order = send_order()
    ball = [k for k in order if hops(k) <= 2]
    middle = [k for k in order if 2 < hops(k) <= 4]
    outer = [k for k in order if hops(k) > 4]
    barrier = pltpu.get_barrier_semaphore()
    for k in ball:
        pl.semaphore_signal(barrier, inc=1, device_id=(peer_of(k),), device_id_type=MESH)

    rows = lists_ref.shape[1]
    owned = cent.shape[0]
    lists_copy.wait()
    ids_copy.wait()
    lists = lists_ref[...]
    owner = lists // owned
    local = (lists - owner * owned).astype(F32)
    ids = ids_ref[...].astype(F32)
    mine = owner == iota((N, rows), 0)
    earlier = (iota((rows, rows), 0) < iota((rows, rows), 1)).astype(BF16)
    count = mm(mine.astype(BF16), earlier)
    lane = iota((N, 128), 1)
    meta = jnp.zeros((N, 128), F32)
    picks = []
    for s in range(SLOTS):
        pick = mine & (count == float(s))
        l_of = jnp.sum(jnp.where(pick, local + 1.0, 0.0), axis=1, keepdims=True) - 1.0
        i_of = jnp.sum(jnp.where(pick, ids, 0.0), axis=1, keepdims=True)
        meta = jnp.where(lane == s, l_of, meta)
        meta = jnp.where(lane == SLOTS + s, i_of, meta)
        picks.append(pick.astype(BF16))
    msend[...] = meta.reshape(N, 1, 128)
    pick_all = jnp.concatenate(picks, axis=0)

    emb_copy.wait()
    rot_copy.start()
    cent_copy.start()
    width = emb.shape[1]
    for nb in range(width // 256):
        hi, mid, low = split3(emb[:, nb * 256:(nb + 1) * 256])
        out = mm(pick_all, hi) + mm(pick_all, mid) + mm(pick_all, low)
        for j in range(2):
            send[pl.ds(nb * 2 + j, SLOTS * N, stride=8), :] = out[:, j * 128:(j + 1) * 128]

    mrecv[pl.ds(me, 1)] = msend[pl.ds(me, 1)]
    for s in range(SLOTS):
        at = pl.ds(pl.multiple_of((s * N + me) * 8, 8), 8)
        recv[at, :] = send[at, :]

    pl.semaphore_wait(barrier, len(ball))
    def send_meta(k):
        peer = peer_of(k)
        pltpu.make_async_remote_copy(
            src_ref=msend.at[pl.ds(peer, 1)], dst_ref=mrecv.at[pl.ds(me, 1)],
            send_sem=msem.at[0], recv_sem=msem.at[1], device_id=(peer,), device_id_type=MESH,
        ).start()

    def send_row(s, k):
        peer = peer_of(k)
        pltpu.make_async_remote_copy(
            src_ref=send.at[pl.ds(pl.multiple_of((s * N + peer) * 8, 8), 8)],
            dst_ref=recv.at[pl.ds(pl.multiple_of((s * N + me) * 8, 8), 8)],
            send_sem=ssem.at[0], recv_sem=rsem.at[s], device_id=(peer,), device_id_type=MESH,
        ).start()

    def send_rows(ks, first, end):
        def slot(s, carry):
            for k in ks:
                send_row(s, k)
            return carry

        lax.fori_loop(first, end, slot, 0)

    for k in ball:
        pl.semaphore_signal(wider.at[0], inc=1, device_id=(peer_of(k),), device_id_type=MESH)
    for k in ball:
        send_meta(k)
    send_rows(ball, 0, NEAR_SLOTS)
    pl.semaphore_wait(wider.at[0], len(ball))
    for k in ball:
        pl.semaphore_signal(wider.at[1], inc=1, device_id=(peer_of(k),), device_id_type=MESH)
    for k in middle:
        send_meta(k)
    send_rows(middle, 0, 1)
    pl.semaphore_wait(wider.at[1], len(ball))
    for k in outer:
        send_meta(k)
    send_rows(outer, 0, 1)
    send_rows(outer + middle, 1, NEAR_SLOTS)
    send_rows(order, NEAR_SLOTS, SLOTS)

    rot_copy.wait()
    for nb in range(width // 256):
        at = slice(nb * 256, (nb + 1) * 256)
        hi, low = split2(rot[:, at])
        rot_hi[:, at] = hi
        rot_lo[:, at] = low

    m_all = msend.at[pl.ds(0, N - 1)]
    pltpu.make_async_copy(m_all, m_all, msem.at[1]).wait()
    got = mrecv[...].reshape(N, 128)
    got_t = got.T
    src_col = iota((N, 1), 0).astype(F32)
    src_row = iota((1, N), 1).astype(F32)
    list_cols = [got[:, s:s + 1] for s in range(SLOTS)]
    list_rows = [got_t[s:s + 1, :] for s in range(SLOTS)]

    def keys(lists_of, src):
        return [jnp.where(v >= 0, v * float(SLOTS * N) + src * float(SLOTS) + float(s), BIG)
                for s, v in enumerate(lists_of)]

    key_cols = keys(list_cols, src_col)
    key_rows = keys(list_rows, src_row)
    q_lane = iota((N, owned), 1).astype(F32)
    pid = jnp.zeros((1, owned), F32)
    off = jnp.zeros((1, owned), F32)
    for s in range(SLOTS):
        by_row = jnp.zeros((N, N), F32)
        by_col = jnp.zeros((N, N), F32)
        for t in range(SLOTS):
            by_row += (key_cols[t] < key_rows[s]).astype(F32)
            by_col += (key_rows[t] < key_cols[s]).astype(F32)
        at_row = jnp.where(list_rows[s] >= 0, jnp.sum(by_row, axis=0, keepdims=True), BIG)
        at_col = jnp.where(list_cols[s] >= 0, jnp.sum(by_col, axis=1, keepdims=True), BIG)
        pos[s:s + 1, :] = at_row
        id_col = got[:, SLOTS + s:SLOTS + s + 1] + 1.0
        pid += jnp.sum(jnp.where(at_col == q_lane, id_col, 0.0), axis=0, keepdims=True)
        off += jnp.sum((key_cols[s] < q_lane * float(SLOTS * N)).astype(F32), axis=0, keepdims=True)
    pids_ref[...] = (pid - 1.0).astype(jnp.int32)
    offs_ref[...] = off.astype(jnp.int32)

    cent_copy.wait()
    onehot = jnp.concatenate([(v == q_lane).astype(BF16) for v in list_cols], axis=0)
    for nb in range(width // 256):
        hi, mid, low = split3(cent[:, nb * 256:(nb + 1) * 256])
        cg[:, nb * 256:(nb + 1) * 256] = mm(onehot, hi) + mm(onehot, mid) + mm(onehot, low)

    packed_ref[...] = jnp.zeros(packed_ref.shape, F32)
    q_sub = iota((SLOTS * N, N), 0).astype(F32)

    def chunk(s, carry):
        r_all = recv.at[pl.ds(0, (N - 1) * 8)]
        pltpu.make_async_copy(r_all, r_all, rsem.at[s]).wait()
        parts = [recv[pl.ds(s * (N * 8) + j, N, stride=8), :] for j in range(8)]
        resid = jnp.concatenate(parts, axis=1) - cg[pl.ds(pl.multiple_of(s * N, N), N), :]
        hi, low = split2(resid)
        both = jnp.concatenate([hi, low], axis=0)
        place = (pos[pl.ds(s, 1), :] == q_sub).astype(BF16)
        place2 = jnp.concatenate([place, place], axis=1)
        for nb in range(width // 256):
            at = slice(nb * 256, (nb + 1) * 256)
            first = mm(both, rot_hi[:, at])
            turned = first[:N] + first[N:] + mm(hi, rot_lo[:, at])
            t_hi, t_lo = split2(turned)
            turned2[0:N, at] = t_hi
            turned2[N:, at] = t_lo
        packed_ref[...] += mm(place2, turned2[...])
        return carry

    lax.fori_loop(0, SLOTS, chunk, 0)
    s_all = send.at[pl.ds(0, SLOTS * (N - 1) * 8)]
    pltpu.make_async_copy(s_all, s_all, ssem.at[0]).wait()
    pltpu.make_async_copy(m_all, m_all, msem.at[0]).wait()


def write_out(packed_vm, pids_vm, offs_vm, packed_ref, pids_ref, offs_ref, sem):
    pairs = ((packed_vm, packed_ref), (pids_vm, pids_ref), (offs_vm, offs_ref))
    copies = [pltpu.make_async_copy(a, b, sem.at[i]) for i, (a, b) in enumerate(pairs)]
    for copy in copies:
        copy.start()
    for copy in copies:
        copy.wait()


def local(embeddings, lists, row_ids, centroids, rotation):
    rows, width = embeddings.shape
    owned = centroids.shape[0]
    slots = SLOTS * N
    vm = pl.BlockSpec(memory_space=pltpu.VMEM)
    hbm = pl.BlockSpec(memory_space=pltpu.HBM)
    results = (
        jax.ShapeDtypeStruct((slots, width), F32),
        jax.ShapeDtypeStruct((1, slots), jnp.int32),
        jax.ShapeDtypeStruct((1, owned), jnp.int32),
    )
    in_hbm = [
        pltpu.with_memory_space_constraint(v, pltpu.HBM)
        for v in (lists.reshape(1, rows), row_ids.reshape(1, rows), embeddings, centroids, rotation)
    ]
    held = pl.pallas_call(
        kernel,
        name="exchange",
        out_shape=results,
        in_specs=[hbm] * 5,
        out_specs=(vm, vm, vm),
        scratch_shapes=[
            pltpu.VMEM((1, rows), jnp.int32),
            pltpu.VMEM((1, rows), jnp.int32),
            pltpu.VMEM((rows, width), F32),
            pltpu.VMEM((owned, width), F32),
            pltpu.VMEM((width, width), F32),
            pltpu.VMEM((width, width), BF16),
            pltpu.VMEM((width, width), BF16),
            pltpu.VMEM((slots * 8, 128), F32),
            pltpu.VMEM((slots * 8, 128), F32),
            pltpu.VMEM((N, 1, 128), F32),
            pltpu.VMEM((N, 1, 128), F32),
            pltpu.VMEM((slots, width), F32),
            pltpu.VMEM((8, 128), F32),
            pltpu.VMEM((2 * N, width), BF16),
            pltpu.SemaphoreType.DMA((5,)),
            pltpu.SemaphoreType.DMA((1,)),
            pltpu.SemaphoreType.DMA((SLOTS,)),
            pltpu.SemaphoreType.DMA((2,)),
            pltpu.SemaphoreType.REGULAR((2,)),
        ],
        compiler_params=pltpu.CompilerParams(
            collective_id=0, has_side_effects=True, vmem_limit_bytes=40 << 20
        ),
    )(*in_hbm)
    packed, pids, offs = pl.pallas_call(
        write_out,
        name="write_out",
        out_shape=results,
        in_specs=[vm] * 3,
        out_specs=(hbm,) * 3,
        scratch_shapes=[pltpu.SemaphoreType.DMA((3,))],
        compiler_params=pltpu.CompilerParams(vmem_limit_bytes=4 << 20),
    )(*held)
    return packed, pids.reshape(-1), offs.reshape(-1)


def solution(mesh):
    in_specs = (P("dev", None), P("dev"), P("dev"), P("dev", None), P())
    out_specs = (P("dev", None), P("dev"), P("dev"))
    return jax.shard_map(local, mesh=mesh, in_specs=in_specs, out_specs=out_specs, check_vma=False)
```

```python
import functools
import random

import jax
import jax.numpy as jnp
from jax import lax
from jax.experimental import pallas as pl
from jax.experimental.pallas import tpu as pltpu
from jax.sharding import PartitionSpec as P

MESH = pl.DeviceIdType.MESH
DIMS = (4, 4, 4, 2)
N = 128
SLOTS = 4
F32 = jnp.float32
BF16 = jnp.bfloat16
BIG = float(1 << 20)
RADII = (2, 1, 1, 2)
MID_SLOTS = 1
NEAR_SLOTS = 3


def digits(k):
    return k // 32, k // 8 % 4, k // 2 % 4, k % 2


def hops(k):
    return sum((0, 1, 2, 1)[d] for d in digits(k)[:3])


def send_order():
    ks = list(range(1, N))
    random.Random(1).shuffle(ks)
    return sorted(ks, key=lambda k: -hops(k))


def iota(shape, dim):
    return lax.broadcasted_iota(jnp.int32, shape, dim)


def split3(x):
    hi = x.astype(BF16)
    rest = x - hi.astype(F32)
    mid = rest.astype(BF16)
    low = (rest - mid.astype(F32)).astype(BF16)
    return hi, mid, low


def split2(x):
    hi = x.astype(BF16)
    return hi, (x - hi.astype(F32)).astype(BF16)


def mm(a, b):
    return jnp.dot(a, b, preferred_element_type=F32)


def kernel(lists_hbm, ids_hbm, emb_hbm, cent_hbm, rot_hbm, packed_ref, pids_ref, offs_ref,
           lists_ref, ids_ref, emb, cent, rot, rot_hi, rot_lo, send, recv, msend, mrecv, cg, pos, turned2,
           lsem, ssem, rsem, msem, wider):
    me = lax.axis_index("dev")
    lists_copy = pltpu.make_async_copy(lists_hbm, lists_ref, lsem.at[3])
    ids_copy = pltpu.make_async_copy(ids_hbm, ids_ref, lsem.at[4])
    emb_copy = pltpu.make_async_copy(emb_hbm, emb, lsem.at[0])
    cent_copy = pltpu.make_async_copy(cent_hbm, cent, lsem.at[1])
    rot_copy = pltpu.make_async_copy(rot_hbm, rot, lsem.at[2])
    lists_copy.start()
    ids_copy.start()
    emb_copy.start()

    z, y, x, c = digits(me)
    zs = [((z + d) % 4) * 32 for d in range(4)]
    ys = [((y + d) % 4) * 8 for d in range(4)]
    xs = [((x + d) % 4) * 2 for d in range(4)]
    cs = [c, 1 - c]

    def peer_of(k):
        a, b, e, f = digits(k)
        return zs[a] + ys[b] + xs[e] + cs[f]

    order = send_order()

    def within(radius):
        return [k for k in order if hops(k) <= radius]

    barrier = pltpu.get_barrier_semaphore()
    for k in within(RADII[0]):
        pl.semaphore_signal(barrier, inc=1, device_id=(peer_of(k),), device_id_type=MESH)

    rows = lists_ref.shape[1]
    owned = cent.shape[0]
    lists_copy.wait()
    ids_copy.wait()
    lists = lists_ref[...]
    owner = lists // owned
    local = (lists - owner * owned).astype(F32)
    ids = ids_ref[...].astype(F32)
    mine = owner == iota((N, rows), 0)
    earlier = (iota((rows, rows), 0) < iota((rows, rows), 1)).astype(BF16)
    count = mm(mine.astype(BF16), earlier)
    masks = [mine & (count == float(s)) for s in range(SLOTS)]
    picks = [v.astype(BF16) for v in masks]
    pick_all = jnp.concatenate(picks, axis=0)

    emb_copy.wait()
    rot_copy.start()
    cent_copy.start()
    width = emb.shape[1]
    for nb in range(width // 256):
        hi, mid, low = split3(emb[:, nb * 256:(nb + 1) * 256])
        out = mm(pick_all, hi) + mm(pick_all, mid) + mm(pick_all, low)
        for j in range(2):
            send[pl.ds(nb * 2 + j, SLOTS * N, stride=8), :] = out[:, j * 128:(j + 1) * 128]

    for s in range(SLOTS):
        at = pl.ds(pl.multiple_of((s * N + me) * 8, 8), 8)
        recv[at, :] = send[at, :]

    pl.semaphore_wait(barrier, len(within(RADII[0])))
    def send_meta(k):
        peer = peer_of(k)
        pltpu.make_async_remote_copy(
            src_ref=msend.at[pl.ds(peer, 1)], dst_ref=mrecv.at[pl.ds(me, 1)],
            send_sem=msem.at[0], recv_sem=msem.at[1], device_id=(peer,), device_id_type=MESH,
        ).start()

    def send_row(s, k):
        peer = peer_of(k)
        pltpu.make_async_remote_copy(
            src_ref=send.at[pl.ds(pl.multiple_of((s * N + peer) * 8, 8), 8)],
            dst_ref=recv.at[pl.ds(pl.multiple_of((s * N + me) * 8, 8), 8)],
            send_sem=ssem.at[0], recv_sem=rsem.at[s], device_id=(peer,), device_id_type=MESH,
        ).start()

    def send_rows(ks, first, end):
        def slot(s, carry):
            for k in ks:
                send_row(s, k)
            return carry

        lax.fori_loop(first, end, slot, 0)

    def build_meta():
        lane = iota((N, 128), 1)
        meta = jnp.zeros((N, 128), F32)
        for s, pick in enumerate(masks):
            l_of = jnp.sum(jnp.where(pick, local + 1.0, 0.0), axis=1, keepdims=True) - 1.0
            i_of = jnp.sum(jnp.where(pick, ids, 0.0), axis=1, keepdims=True)
            meta = jnp.where(lane == s, l_of, meta)
            meta = jnp.where(lane == SLOTS + s, i_of, meta)
        msend[...] = meta.reshape(N, 1, 128)
        mrecv[pl.ds(me, 1)] = msend[pl.ds(me, 1)]

    def signal_round(i):
        for k in within(RADII[i + 1]):
            pl.semaphore_signal(wider.at[i], inc=1, device_id=(peer_of(k),), device_id_type=MESH)

    rounds = len(RADII) - 1
    reached, metas = 0, []
    for i in range(rounds + 1):
        if i:
            pl.semaphore_wait(wider.at[i - 1], len(within(RADII[i])))
        if i < rounds:
            signal_round(i)
        known = reached + RADII[i]
        fresh = [k for k in order if reached - (not i) < hops(k) <= known]
        send_rows(fresh, 0, NEAR_SLOTS if known <= 2 else MID_SLOTS)
        if i == 0:
            build_meta()
        metas += fresh
        if i:
            for k in metas:
                send_meta(k)
            metas = []
        reached = known
    send_rows([k for k in order if hops(k) > 2], MID_SLOTS, NEAR_SLOTS)
    send_rows(order, NEAR_SLOTS, SLOTS)

    rot_copy.wait()
    for nb in range(width // 256):
        at = slice(nb * 256, (nb + 1) * 256)
        hi, low = split2(rot[:, at])
        rot_hi[:, at] = hi
        rot_lo[:, at] = low

    m_all = msend.at[pl.ds(0, N - 1)]
    pltpu.make_async_copy(m_all, m_all, msem.at[1]).wait()
    got = mrecv[...].reshape(N, 128)
    got_t = got.T
    src_col = iota((N, 1), 0).astype(F32)
    src_row = iota((1, N), 1).astype(F32)
    list_cols = [got[:, s:s + 1] for s in range(SLOTS)]
    list_rows = [got_t[s:s + 1, :] for s in range(SLOTS)]

    def keys(lists_of, src):
        return [jnp.where(v >= 0, v * float(SLOTS * N) + src * float(SLOTS) + float(s), BIG)
                for s, v in enumerate(lists_of)]

    key_cols = keys(list_cols, src_col)
    key_rows = keys(list_rows, src_row)
    q_lane = iota((N, owned), 1).astype(F32)
    pid = jnp.zeros((1, owned), F32)
    off = jnp.zeros((1, owned), F32)
    for s in range(SLOTS):
        by_row = jnp.zeros((N, N), F32)
        by_col = jnp.zeros((N, N), F32)
        for t in range(SLOTS):
            by_row += (key_cols[t] < key_rows[s]).astype(F32)
            by_col += (key_rows[t] < key_cols[s]).astype(F32)
        at_row = jnp.where(list_rows[s] >= 0, jnp.sum(by_row, axis=0, keepdims=True), BIG)
        at_col = jnp.where(list_cols[s] >= 0, jnp.sum(by_col, axis=1, keepdims=True), BIG)
        pos[s:s + 1, :] = at_row
        id_col = got[:, SLOTS + s:SLOTS + s + 1] + 1.0
        pid += jnp.sum(jnp.where(at_col == q_lane, id_col, 0.0), axis=0, keepdims=True)
        off += jnp.sum((key_cols[s] < q_lane * float(SLOTS * N)).astype(F32), axis=0, keepdims=True)
    pids_ref[...] = (pid - 1.0).astype(jnp.int32)
    offs_ref[...] = off.astype(jnp.int32)

    cent_copy.wait()
    onehot = jnp.concatenate([(v == q_lane).astype(BF16) for v in list_cols], axis=0)
    for nb in range(width // 256):
        hi, mid, low = split3(cent[:, nb * 256:(nb + 1) * 256])
        cg[:, nb * 256:(nb + 1) * 256] = mm(onehot, hi) + mm(onehot, mid) + mm(onehot, low)

    packed_ref[...] = jnp.zeros(packed_ref.shape, F32)
    q_sub = iota((SLOTS * N, N), 0).astype(F32)

    def chunk(s, carry):
        r_all = recv.at[pl.ds(0, (N - 1) * 8)]
        pltpu.make_async_copy(r_all, r_all, rsem.at[s]).wait()
        parts = [recv[pl.ds(s * (N * 8) + j, N, stride=8), :] for j in range(8)]
        resid = jnp.concatenate(parts, axis=1) - cg[pl.ds(pl.multiple_of(s * N, N), N), :]
        hi, low = split2(resid)
        both = jnp.concatenate([hi, low], axis=0)
        place = (pos[pl.ds(s, 1), :] == q_sub).astype(BF16)
        place2 = jnp.concatenate([place, place], axis=1)
        for nb in range(width // 256):
            at = slice(nb * 256, (nb + 1) * 256)
            first = mm(both, rot_hi[:, at])
            turned = first[:N] + first[N:] + mm(hi, rot_lo[:, at])
            t_hi, t_lo = split2(turned)
            turned2[0:N, at] = t_hi
            turned2[N:, at] = t_lo
        packed_ref[...] += mm(place2, turned2[...])
        return carry

    lax.fori_loop(0, SLOTS, chunk, 0)
    s_all = send.at[pl.ds(0, SLOTS * (N - 1) * 8)]
    pltpu.make_async_copy(s_all, s_all, ssem.at[0]).wait()
    pltpu.make_async_copy(m_all, m_all, msem.at[0]).wait()


def write_out(packed_vm, pids_vm, offs_vm, packed_ref, pids_ref, offs_ref, sem):
    pairs = ((packed_vm, packed_ref), (pids_vm, pids_ref), (offs_vm, offs_ref))
    copies = [pltpu.make_async_copy(a, b, sem.at[i]) for i, (a, b) in enumerate(pairs)]
    for copy in copies:
        copy.start()
    for copy in copies:
        copy.wait()


def local(embeddings, lists, row_ids, centroids, rotation):
    rows, width = embeddings.shape
    owned = centroids.shape[0]
    slots = SLOTS * N
    vm = pl.BlockSpec(memory_space=pltpu.VMEM)
    hbm = pl.BlockSpec(memory_space=pltpu.HBM)
    results = (
        jax.ShapeDtypeStruct((slots, width), F32),
        jax.ShapeDtypeStruct((1, slots), jnp.int32),
        jax.ShapeDtypeStruct((1, owned), jnp.int32),
    )
    in_hbm = [
        pltpu.with_memory_space_constraint(v, pltpu.HBM)
        for v in (lists.reshape(1, rows), row_ids.reshape(1, rows), embeddings, centroids, rotation)
    ]
    held = pl.pallas_call(
        kernel,
        name="exchange",
        out_shape=results,
        in_specs=[hbm] * 5,
        out_specs=(vm, vm, vm),
        scratch_shapes=[
            pltpu.VMEM((1, rows), jnp.int32),
            pltpu.VMEM((1, rows), jnp.int32),
            pltpu.VMEM((rows, width), F32),
            pltpu.VMEM((owned, width), F32),
            pltpu.VMEM((width, width), F32),
            pltpu.VMEM((width, width), BF16),
            pltpu.VMEM((width, width), BF16),
            pltpu.VMEM((slots * 8, 128), F32),
            pltpu.VMEM((slots * 8, 128), F32),
            pltpu.VMEM((N, 1, 128), F32),
            pltpu.VMEM((N, 1, 128), F32),
            pltpu.VMEM((slots, width), F32),
            pltpu.VMEM((8, 128), F32),
            pltpu.VMEM((2 * N, width), BF16),
            pltpu.SemaphoreType.DMA((5,)),
            pltpu.SemaphoreType.DMA((1,)),
            pltpu.SemaphoreType.DMA((SLOTS,)),
            pltpu.SemaphoreType.DMA((2,)),
            pltpu.SemaphoreType.REGULAR((len(RADII) - 1,)),
        ],
        compiler_params=pltpu.CompilerParams(
            collective_id=0, has_side_effects=True, vmem_limit_bytes=40 << 20
        ),
    )(*in_hbm)
    packed, pids, offs = pl.pallas_call(
        write_out,
        name="write_out",
        out_shape=results,
        in_specs=[vm] * 3,
        out_specs=(hbm,) * 3,
        scratch_shapes=[pltpu.SemaphoreType.DMA((3,))],
        compiler_params=pltpu.CompilerParams(vmem_limit_bytes=4 << 20),
    )(*held)
    return packed, pids.reshape(-1), offs.reshape(-1)


def solution(mesh):
    in_specs = (P("dev", None), P("dev"), P("dev"), P("dev", None), P())
    out_specs = (P("dev", None), P("dev"), P("dev"))
    return jax.shard_map(local, mesh=mesh, in_specs=in_specs, out_specs=out_specs, check_vma=False)
```

```python
import functools
import random

import jax
import jax.numpy as jnp
from jax import lax
from jax.experimental import pallas as pl
from jax.experimental.pallas import tpu as pltpu
from jax.sharding import PartitionSpec as P

MESH = pl.DeviceIdType.MESH
DIMS = (4, 4, 4, 2)
N = 128
SLOTS = 4
F32 = jnp.float32
BF16 = jnp.bfloat16
BIG = float(1 << 20)
RADII = (2, 1, 3)
MID_SLOTS = 1
NEAR_SLOTS = 3


def digits(k):
    return k // 32, k // 8 % 4, k // 2 % 4, k % 2


def hops(k):
    return sum((0, 1, 2, 1)[d] for d in digits(k)[:3])


def send_order():
    ks = list(range(1, N))
    random.Random(1).shuffle(ks)
    return sorted(ks, key=lambda k: -hops(k))


def iota(shape, dim):
    return lax.broadcasted_iota(jnp.int32, shape, dim)


def split3(x):
    hi = x.astype(BF16)
    rest = x - hi.astype(F32)
    mid = rest.astype(BF16)
    low = (rest - mid.astype(F32)).astype(BF16)
    return hi, mid, low


def split2(x):
    hi = x.astype(BF16)
    return hi, (x - hi.astype(F32)).astype(BF16)


def mm(a, b):
    return jnp.dot(a, b, preferred_element_type=F32)


def kernel(lists_hbm, ids_hbm, emb_hbm, cent_hbm, rot_hbm, packed_ref, pids_ref, offs_ref,
           lists_ref, ids_ref, emb, cent, rot, rot_hi, rot_lo, send, recv, msend, mrecv, cg, pos, turned2,
           lsem, ssem, rsem, msem, wider):
    me = lax.axis_index("dev")
    lists_copy = pltpu.make_async_copy(lists_hbm, lists_ref, lsem.at[3])
    ids_copy = pltpu.make_async_copy(ids_hbm, ids_ref, lsem.at[4])
    emb_copy = pltpu.make_async_copy(emb_hbm, emb, lsem.at[0])
    cent_copy = pltpu.make_async_copy(cent_hbm, cent, lsem.at[1])
    rot_copy = pltpu.make_async_copy(rot_hbm, rot, lsem.at[2])
    lists_copy.start()
    ids_copy.start()
    emb_copy.start()

    z, y, x, c = digits(me)
    zs = [((z + d) % 4) * 32 for d in range(4)]
    ys = [((y + d) % 4) * 8 for d in range(4)]
    xs = [((x + d) % 4) * 2 for d in range(4)]
    cs = [c, 1 - c]

    def peer_of(k):
        a, b, e, f = digits(k)
        return zs[a] + ys[b] + xs[e] + cs[f]

    order = send_order()

    def within(radius):
        return [k for k in order if hops(k) <= radius]

    barrier = pltpu.get_barrier_semaphore()
    for k in within(RADII[0]):
        pl.semaphore_signal(barrier, inc=1, device_id=(peer_of(k),), device_id_type=MESH)

    rows = lists_ref.shape[1]
    owned = cent.shape[0]
    lists_copy.wait()
    ids_copy.wait()
    lists = lists_ref[...]
    owner = lists // owned
    local = (lists - owner * owned).astype(F32)
    ids = ids_ref[...].astype(F32)
    mine = owner == iota((N, rows), 0)
    earlier = (iota((rows, rows), 0) < iota((rows, rows), 1)).astype(BF16)
    count = mm(mine.astype(BF16), earlier)
    masks = [mine & (count == float(s)) for s in range(SLOTS)]
    picks = [v.astype(BF16) for v in masks]
    pick_all = jnp.concatenate(picks, axis=0)

    emb_copy.wait()
    rot_copy.start()
    cent_copy.start()
    width = emb.shape[1]
    for nb in range(width // 256):
        hi, mid, low = split3(emb[:, nb * 256:(nb + 1) * 256])
        out = mm(pick_all, hi) + mm(pick_all, mid) + mm(pick_all, low)
        for j in range(2):
            send[pl.ds(nb * 2 + j, SLOTS * N, stride=8), :] = out[:, j * 128:(j + 1) * 128]

    for s in range(SLOTS):
        at = pl.ds(pl.multiple_of((s * N + me) * 8, 8), 8)
        recv[at, :] = send[at, :]

    pl.semaphore_wait(barrier, len(within(RADII[0])))
    def send_meta(k):
        peer = peer_of(k)
        pltpu.make_async_remote_copy(
            src_ref=msend.at[pl.ds(peer, 1)], dst_ref=mrecv.at[pl.ds(me, 1)],
            send_sem=msem.at[0], recv_sem=msem.at[1], device_id=(peer,), device_id_type=MESH,
        ).start()

    def send_row(s, k):
        peer = peer_of(k)
        pltpu.make_async_remote_copy(
            src_ref=send.at[pl.ds(pl.multiple_of((s * N + peer) * 8, 8), 8)],
            dst_ref=recv.at[pl.ds(pl.multiple_of((s * N + me) * 8, 8), 8)],
            send_sem=ssem.at[0], recv_sem=rsem.at[s], device_id=(peer,), device_id_type=MESH,
        ).start()

    def send_rows(ks, first, end):
        def slot(s, carry):
            for k in ks:
                send_row(s, k)
            return carry

        lax.fori_loop(first, end, slot, 0)

    def build_meta():
        lane = iota((N, 128), 1)
        meta = jnp.zeros((N, 128), F32)
        for s, pick in enumerate(masks):
            l_of = jnp.sum(jnp.where(pick, local + 1.0, 0.0), axis=1, keepdims=True) - 1.0
            i_of = jnp.sum(jnp.where(pick, ids, 0.0), axis=1, keepdims=True)
            meta = jnp.where(lane == s, l_of, meta)
            meta = jnp.where(lane == SLOTS + s, i_of, meta)
        msend[...] = meta.reshape(N, 1, 128)
        mrecv[pl.ds(me, 1)] = msend[pl.ds(me, 1)]

    def signal_round(i):
        for k in within(RADII[i + 1]):
            pl.semaphore_signal(wider.at[i], inc=1, device_id=(peer_of(k),), device_id_type=MESH)

    rounds = len(RADII) - 1
    reached, metas = 0, []
    for i in range(rounds + 1):
        if i:
            pl.semaphore_wait(wider.at[i - 1], len(within(RADII[i])))
        if i < rounds:
            signal_round(i)
        known = reached + RADII[i]
        fresh = [k for k in order if reached - (not i) < hops(k) <= known]
        send_rows(fresh, 0, NEAR_SLOTS if known <= 2 else MID_SLOTS)
        if i == 0:
            build_meta()
        metas += fresh
        if i:
            for k in metas:
                send_meta(k)
            metas = []
        reached = known
    send_rows([k for k in order if hops(k) > 2], MID_SLOTS, NEAR_SLOTS)
    send_rows(order, NEAR_SLOTS, SLOTS)

    rot_copy.wait()
    for nb in range(width // 256):
        at = slice(nb * 256, (nb + 1) * 256)
        hi, low = split2(rot[:, at])
        rot_hi[:, at] = hi
        rot_lo[:, at] = low

    m_all = msend.at[pl.ds(0, N - 1)]
    pltpu.make_async_copy(m_all, m_all, msem.at[1]).wait()
    got = mrecv[...].reshape(N, 128)
    got_t = got.T
    src_col = iota((N, 1), 0).astype(F32)
    src_row = iota((1, N), 1).astype(F32)
    list_cols = [got[:, s:s + 1] for s in range(SLOTS)]
    list_rows = [got_t[s:s + 1, :] for s in range(SLOTS)]

    def keys(lists_of, src):
        return [jnp.where(v >= 0, v * float(SLOTS * N) + src * float(SLOTS) + float(s), BIG)
                for s, v in enumerate(lists_of)]

    key_cols = keys(list_cols, src_col)
    key_rows = keys(list_rows, src_row)
    q_lane = iota((N, owned), 1).astype(F32)
    pid = jnp.zeros((1, owned), F32)
    off = jnp.zeros((1, owned), F32)
    for s in range(SLOTS):
        by_row = jnp.zeros((N, N), F32)
        by_col = jnp.zeros((N, N), F32)
        for t in range(SLOTS):
            by_row += (key_cols[t] < key_rows[s]).astype(F32)
            by_col += (key_rows[t] < key_cols[s]).astype(F32)
        at_row = jnp.where(list_rows[s] >= 0, jnp.sum(by_row, axis=0, keepdims=True), BIG)
        at_col = jnp.where(list_cols[s] >= 0, jnp.sum(by_col, axis=1, keepdims=True), BIG)
        pos[s:s + 1, :] = at_row
        id_col = got[:, SLOTS + s:SLOTS + s + 1] + 1.0
        pid += jnp.sum(jnp.where(at_col == q_lane, id_col, 0.0), axis=0, keepdims=True)
        off += jnp.sum((key_cols[s] < q_lane * float(SLOTS * N)).astype(F32), axis=0, keepdims=True)
    pids_ref[...] = (pid - 1.0).astype(jnp.int32)
    offs_ref[...] = off.astype(jnp.int32)

    cent_copy.wait()
    onehot = jnp.concatenate([(v == q_lane).astype(BF16) for v in list_cols], axis=0)
    for nb in range(width // 256):
        hi, mid, low = split3(cent[:, nb * 256:(nb + 1) * 256])
        cg[:, nb * 256:(nb + 1) * 256] = mm(onehot, hi) + mm(onehot, mid) + mm(onehot, low)

    packed_ref[...] = jnp.zeros(packed_ref.shape, F32)
    q_sub = iota((SLOTS * N, N), 0).astype(F32)

    def chunk(s, carry):
        r_all = recv.at[pl.ds(0, (N - 1) * 8)]
        pltpu.make_async_copy(r_all, r_all, rsem.at[s]).wait()
        parts = [recv[pl.ds(s * (N * 8) + j, N, stride=8), :] for j in range(8)]
        resid = jnp.concatenate(parts, axis=1) - cg[pl.ds(pl.multiple_of(s * N, N), N), :]
        hi, low = split2(resid)
        both = jnp.concatenate([hi, low], axis=0)
        place = (pos[pl.ds(s, 1), :] == q_sub).astype(BF16)
        place2 = jnp.concatenate([place, place], axis=1)
        for nb in range(width // 256):
            at = slice(nb * 256, (nb + 1) * 256)
            first = mm(both, rot_hi[:, at])
            turned = first[:N] + first[N:] + mm(hi, rot_lo[:, at])
            t_hi, t_lo = split2(turned)
            turned2[0:N, at] = t_hi
            turned2[N:, at] = t_lo
        packed_ref[...] += mm(place2, turned2[...])
        return carry

    lax.fori_loop(0, SLOTS, chunk, 0)
    s_all = send.at[pl.ds(0, SLOTS * (N - 1) * 8)]
    pltpu.make_async_copy(s_all, s_all, ssem.at[0]).wait()
    pltpu.make_async_copy(m_all, m_all, msem.at[0]).wait()


def write_out(packed_vm, pids_vm, offs_vm, packed_ref, pids_ref, offs_ref, sem):
    pairs = ((packed_vm, packed_ref), (pids_vm, pids_ref), (offs_vm, offs_ref))
    copies = [pltpu.make_async_copy(a, b, sem.at[i]) for i, (a, b) in enumerate(pairs)]
    for copy in copies:
        copy.start()
    for copy in copies:
        copy.wait()


def local(embeddings, lists, row_ids, centroids, rotation):
    rows, width = embeddings.shape
    owned = centroids.shape[0]
    slots = SLOTS * N
    vm = pl.BlockSpec(memory_space=pltpu.VMEM)
    hbm = pl.BlockSpec(memory_space=pltpu.HBM)
    results = (
        jax.ShapeDtypeStruct((slots, width), F32),
        jax.ShapeDtypeStruct((1, slots), jnp.int32),
        jax.ShapeDtypeStruct((1, owned), jnp.int32),
    )
    in_hbm = [
        pltpu.with_memory_space_constraint(v, pltpu.HBM)
        for v in (lists.reshape(1, rows), row_ids.reshape(1, rows), embeddings, centroids, rotation)
    ]
    held = pl.pallas_call(
        kernel,
        name="exchange",
        out_shape=results,
        in_specs=[hbm] * 5,
        out_specs=(vm, vm, vm),
        scratch_shapes=[
            pltpu.VMEM((1, rows), jnp.int32),
            pltpu.VMEM((1, rows), jnp.int32),
            pltpu.VMEM((rows, width), F32),
            pltpu.VMEM((owned, width), F32),
            pltpu.VMEM((width, width), F32),
            pltpu.VMEM((width, width), BF16),
            pltpu.VMEM((width, width), BF16),
            pltpu.VMEM((slots * 8, 128), F32),
            pltpu.VMEM((slots * 8, 128), F32),
            pltpu.VMEM((N, 1, 128), F32),
            pltpu.VMEM((N, 1, 128), F32),
            pltpu.VMEM((slots, width), F32),
            pltpu.VMEM((8, 128), F32),
            pltpu.VMEM((2 * N, width), BF16),
            pltpu.SemaphoreType.DMA((5,)),
            pltpu.SemaphoreType.DMA((1,)),
            pltpu.SemaphoreType.DMA((SLOTS,)),
            pltpu.SemaphoreType.DMA((2,)),
            pltpu.SemaphoreType.REGULAR((len(RADII) - 1,)),
        ],
        compiler_params=pltpu.CompilerParams(
            collective_id=0, has_side_effects=True, vmem_limit_bytes=40 << 20
        ),
    )(*in_hbm)
    packed, pids, offs = pl.pallas_call(
        write_out,
        name="write_out",
        out_shape=results,
        in_specs=[vm] * 3,
        out_specs=(hbm,) * 3,
        scratch_shapes=[pltpu.SemaphoreType.DMA((3,))],
        compiler_params=pltpu.CompilerParams(vmem_limit_bytes=4 << 20),
    )(*held)
    return packed, pids.reshape(-1), offs.reshape(-1)


def solution(mesh):
    in_specs = (P("dev", None), P("dev"), P("dev"), P("dev", None), P())
    out_specs = (P("dev", None), P("dev"), P("dev"))
    return jax.shard_map(local, mesh=mesh, in_specs=in_specs, out_specs=out_specs, check_vma=False)
```
